32 devices in a mesh: seq: 8 (over z, y), rep: 4 (over x, core).
Axes of the slice: x: 2, y: 2, z: 4, core: 2. Of those that a mesh axis runs over, the one named last changes fastest.
Arguments:
- query_rows: bfloat16 [12288, 1024], P(('seq', 'rep')), may hold values from -6 to 6
- key_rows: bfloat16 [12288, 128], P(('seq', 'rep')), may hold values from -6 to 6
- value_rows: bfloat16 [12288, 128], P(('seq', 'rep')), may hold values from -6 to 6
- out_grad: bfloat16 [12288, 1024], P(('seq', 'rep')), may hold values from -1.5 to 1.5
- logsumexp: float32 [8, 12288], P(None, ('seq', 'rep')), may hold values from 1 to 3
- row_delta: float32 [8, 12288], P(None, ('seq', 'rep')), may hold values from -8 to 8
- doc_lengths: int32 [31], replicated, may hold values from 1 to 1537, as said below
Outputs:
- query_grad: bfloat16 [12288, 1024], P(('seq', 'rep'))
- key_grad: bfloat16 [12288, 128], P(('seq', 'rep'))
- value_grad: bfloat16 [12288, 128], P(('seq', 'rep'))
The draws below stay inside these ranges and needn't reach their ends.
Inputs may be any that keep to these rules, and one draw needn't show every extreme that they name: `doc_lengths`: 31 document lengths in pack order, summing to 12288; so every document lies within 5 consecutive aligned blocks of 384 positions.
All inputs are finite; a program needn't handle non-finite values.
Results may differ from the reference program's by a relative error of at most 0.019.
Values may be sent and summed in bfloat16 or wider, within the bound.
A program may use at most 64 MiB of HBM per device.

```python
import jax
import jax.numpy as jnp
from jax import lax

HEADS = 8
HD = 128
TOK_DEV = 384
REACH = 4
TOKENS = 12288
N_SEQ = 8
N_REP = 4


def draw_doc_lengths(key, part):
    blocks = N_SEQ * N_REP
    frames = 2 * blocks // REACH
    span = REACH * TOK_DEV // 2
    short_most = TOK_DEV // 4
    base_key = jax.random.fold_in(key, 11)
    key_start, key_short, key_pick = jax.random.split(base_key, 3)
    starts = jax.random.randint(key_start, (frames + 1,), short_most, span).astype(jnp.int32)
    shorts = jax.random.randint(key_short, (frames + 1,), 1, short_most + 1).astype(jnp.int32)
    chosen = jax.random.randint(key_pick, (), 1, frames - 1).astype(jnp.int32)
    index = jnp.arange(frames + 1, dtype=jnp.int32)
    starts = jnp.where(index == chosen + 1, span - 1, starts)
    starts = jnp.where(index == chosen - 1, jnp.minimum(starts, span - 4 - short_most), starts)
    starts = jnp.where(index == chosen, -3, starts)
    shorts = jnp.where(index == chosen + 1, 1, shorts)
    starts = jnp.where((index == 0) | (index == frames), 0, starts)
    long_start = index * span + starts
    short_start = long_start - shorts
    inner = jnp.stack([short_start[1:frames], long_start[1:frames]], 1).reshape(-1)
    bounds = jnp.concatenate([jnp.zeros((1,), jnp.int32), inner.astype(jnp.int32), jnp.full((1,), TOKENS, jnp.int32)])
    return (bounds[1:] - bounds[:-1]).astype(jnp.int32)


def block_levels(rng, shape, cuts, low, largest):
    def one(position, blocks):
        steps = jax.random.uniform(jax.random.fold_in(jax.random.fold_in(rng, 6), position), (blocks,), jnp.float32, low / len(cuts), largest / len(cuts))
        return jnp.repeat(jnp.exp(steps), shape[position] // blocks).reshape((-1,) + (1,) * (len(shape) - position - 1))

    gain = one(*cuts[0])
    for cut in cuts[1:]:
        gain = gain * one(*cut)
    return gain


def centred(key, dims, width, most, cuts=(), kind=jnp.bfloat16):
    values = width * jax.random.normal(key, dims, jnp.float32)
    if cuts:
        values = values * block_levels(key, dims, cuts, -0.22, 0.18)
    return jnp.clip(values, -most, most).astype(kind)


def setup_inputs(seed: int = 0) -> dict:
    seeds = jax.random.split(jax.random.key(seed), 8)
    query_rows = centred(seeds[0], (TOKENS, HEADS * HD), 1.0, 6.0, ((0, 32),))
    key_rows = centred(seeds[1], (TOKENS, HD), 1.0, 6.0, ((0, 32),))
    value_rows = centred(seeds[2], (TOKENS, HD), 1.0, 6.0, ((0, 32),))
    out_grad = centred(seeds[3], (TOKENS, HEADS * HD), 0.25, 1.5, ((0, 32),))
    logsumexp = jnp.clip(1.0 + 2.0 * jax.random.uniform(seeds[4], (HEADS, TOKENS), jnp.float32) ** block_levels(seeds[4], (HEADS, TOKENS), ((1, 32),), -0.2, 0.2), 1.0, 3.0)
    row_delta = centred(seeds[5], (HEADS, TOKENS), 2.0, 8.0, ((1, 32),), jnp.float32)
    doc_lengths = draw_doc_lengths(jax.random.fold_in(seeds[7], 71), 0)
    return {"query_rows": query_rows, "key_rows": key_rows, "value_rows": value_rows, "out_grad": out_grad, "logsumexp": logsumexp, "row_delta": row_delta, "doc_lengths": doc_lengths}


def block_grads(query_block, grad_block, stat_block, delta_block, key_block, value_block, query_docs, key_docs, query_pos, key_pos):
    row_count = query_block.shape[0]
    query_heads = query_block.astype(jnp.float32).reshape(row_count, HEADS, HD)
    grad_heads = grad_block.astype(jnp.float32).reshape(row_count, HEADS, HD)
    key_float = key_block.astype(jnp.float32)
    value_float = value_block.astype(jnp.float32)
    score_scale = HD ** -0.5
    scores = jnp.einsum("qhd,kd->hqk", query_heads, key_float) * score_scale
    allowed = (query_docs[:, None] == key_docs[None, :]) & (key_pos[None, :] <= query_pos[:, None])
    probs = jnp.where(allowed[None], jnp.exp(scores - stat_block[:, :, None]), 0.0)
    dprobs = jnp.einsum("qhd,kd->hqk", grad_heads, value_float)
    dscores = probs * (dprobs - delta_block[:, :, None])
    probs_half = probs.astype(jnp.bfloat16).astype(jnp.float32)
    dscores_half = dscores.astype(jnp.bfloat16).astype(jnp.float32)
    query_part = (jnp.einsum("hqk,kd->qhd", dscores_half, key_float) * score_scale).reshape(row_count, HEADS * HD)
    key_part = jnp.einsum("hqk,qhd->kd", dscores_half, query_heads) * score_scale
    value_part = jnp.einsum("hqk,qhd->kd", probs_half, grad_heads)
    return query_part, key_part, value_part


def shifted_blocks(array, distance, filler):
    return jnp.concatenate([filler, array[:-distance]], 0)


def reference(query_rows, key_rows, value_rows, out_grad, logsumexp, row_delta, doc_lengths):
    blocks = N_SEQ * N_REP
    total = blocks * TOK_DEV
    doc_ends = jnp.cumsum(doc_lengths).astype(jnp.int32)
    marks = jnp.zeros((total,), jnp.int32).at[doc_ends[:-1]].add(1)
    docs = jnp.cumsum(marks).astype(jnp.int32).reshape(blocks, TOK_DEV)
    positions = jnp.arange(total, dtype=jnp.int32).reshape(blocks, TOK_DEV)
    queries = query_rows.reshape(blocks, TOK_DEV, HEADS * HD)
    grads = out_grad.reshape(blocks, TOK_DEV, HEADS * HD)
    keys_all = key_rows.reshape(blocks, TOK_DEV, HD)
    values_all = value_rows.reshape(blocks, TOK_DEV, HD)
    stats = logsumexp.reshape(HEADS, blocks, TOK_DEV).transpose(1, 0, 2)
    deltas = row_delta.reshape(HEADS, blocks, TOK_DEV).transpose(1, 0, 2)
    prev_keys = jnp.stack([shifted_blocks(keys_all, step, jnp.zeros_like(keys_all[:step])) for step in range(1, REACH + 1)], 1)
    prev_values = jnp.stack([shifted_blocks(values_all, step, jnp.zeros_like(values_all[:step])) for step in range(1, REACH + 1)], 1)
    prev_docs = jnp.stack([shifted_blocks(docs, step, jnp.full((step, TOK_DEV), -1, jnp.int32)) for step in range(1, REACH + 1)], 1)
    prev_pos = jnp.stack([positions - step * TOK_DEV for step in range(1, REACH + 1)], 1)

    def one_block(block_items):
        query_block, grad_block, stat_block, delta_block, key_block, value_block, doc_block, pos_block, pkey, pvalue, pdoc, ppos = block_items
        query_sum, local_k, local_v = block_grads(query_block, grad_block, stat_block, delta_block, key_block, value_block, doc_block, doc_block, pos_block, pos_block)
        cross_keys = []
        cross_values = []
        for step in range(REACH):
            cross_q, cross_k, cross_v = block_grads(query_block, grad_block, stat_block, delta_block, pkey[step], pvalue[step], doc_block, pdoc[step], pos_block, ppos[step])
            query_sum = query_sum + cross_q
            cross_keys.append(cross_k)
            cross_values.append(cross_v)
        return query_sum, local_k, local_v, jnp.stack(cross_keys, 0), jnp.stack(cross_values, 0)

    query_sum, local_k, local_v, cross_k, cross_v = lax.map(one_block, (queries, grads, stats, deltas, keys_all, values_all, docs, positions, prev_keys, prev_values, prev_docs, prev_pos))
    key_sum = local_k
    value_sum = local_v
    for step in range(1, REACH + 1):
        key_sum = key_sum + jnp.concatenate([cross_k[step:, step - 1], jnp.zeros_like(cross_k[:step, step - 1])], 0)
        value_sum = value_sum + jnp.concatenate([cross_v[step:, step - 1], jnp.zeros_like(cross_v[:step, step - 1])], 0)
    return (query_sum.reshape(total, HEADS * HD).astype(jnp.bfloat16), key_sum.reshape(total, HD).astype(jnp.bfloat16), value_sum.reshape(total, HD).astype(jnp.bfloat16))
```

```python
import functools
import math

import jax
import jax.numpy as jnp
from jax import lax
from jax.experimental import pallas as pl
from jax.experimental.pallas import tpu as pltpu
from jax.sharding import PartitionSpec as P

REACH = 4
LANES = 128
LOG2E = math.log2(math.e)
MESH = pl.DeviceIdType.MESH


def dot(a, b):
    return jnp.dot(a, b, preferred_element_type=jnp.float32)


def dot_nt(a, b):
    return lax.dot_general(a, b, (((1,), (1,)), ((), ())), preferred_element_type=jnp.float32)


def kernel(
    count,
    per_seq,
    lens_ref,
    q_hbm,
    g_hbm,
    k_ref,
    v_ref,
    lse_ref,
    delta_ref,
    dq_ref,
    dk_ref,
    dv_ref,
    q,
    g,
    kbuf,
    vbuf,
    k_t,
    bias,
    lse2,
    dq_t,
    own_k,
    own_v,
    acc_k,
    acc_v,
    out_k,
    out_v,
    in_k,
    in_v,
    load_sem,
    kv_send,
    kv_recv,
    gr_send,
    gr_recv,
):
    rows, head = k_ref.shape
    heads = q.shape[1] // head
    scale = head**-0.5
    me = lax.axis_index("seq") * per_seq + lax.axis_index("rep")

    def device(index):
        return (lax.div(index, per_seq), lax.rem(index, per_seq))

    load_q = pltpu.make_async_copy(q_hbm, q, load_sem.at[0])
    load_g = pltpu.make_async_copy(g_hbm, g, load_sem.at[1])
    load_q.start()
    load_g.start()

    barrier = pltpu.get_barrier_semaphore()
    for d in range(1, REACH + 1):

        @pl.when(me + d < count)
        def _():
            pl.semaphore_signal(barrier, inc=1, device_id=device(me + d), device_id_type=MESH)

        @pl.when(me >= d)
        def _():
            pl.semaphore_signal(barrier, inc=1, device_id=device(me - d), device_id_type=MESH)

    pl.semaphore_wait(barrier, jnp.minimum(me, REACH) + jnp.minimum(count - 1 - me, REACH))

    def kv_copies(d):
        return [
            pltpu.make_async_remote_copy(
                src_ref=src,
                dst_ref=dst.at[d - 1],
                send_sem=kv_send.at[n, d - 1],
                recv_sem=kv_recv.at[n, d - 1],
                device_id=device(me + d),
                device_id_type=MESH,
            )
            for n, (src, dst) in enumerate(((k_ref, kbuf), (v_ref, vbuf)))
        ]

    def grad_copies(d):
        return [
            pltpu.make_async_remote_copy(
                src_ref=src.at[d - 1],
                dst_ref=dst.at[d - 1],
                send_sem=gr_send.at[n, d - 1],
                recv_sem=gr_recv.at[n, d - 1],
                device_id=device(me - d),
                device_id_type=MESH,
            )
            for n, (src, dst) in enumerate(((out_k, in_k), (out_v, in_v)))
        ]

    for d in range(1, REACH + 1):

        @pl.when(me + d < count)
        def _():
            for copy in kv_copies(d):
                copy.start()

    t_pos = me * rows + lax.broadcasted_iota(jnp.int32, (1, rows), 1)

    def next_doc(j, carry):
        end, start = carry
        end = end + lens_ref[j]
        return end, jnp.where(end <= t_pos, end, start)

    _, start = lax.fori_loop(
        0, lens_ref.shape[0], next_doc, (jnp.int32(0), jnp.zeros((1, rows), jnp.int32))
    )
    lse2[...] = lse_ref[...] * LOG2E

    def set_bias(d):
        u_pos = (me - d) * rows + lax.broadcasted_iota(jnp.int32, (rows, rows), 0)
        bias[...] = jnp.where((u_pos >= start) & (u_pos <= t_pos), 0.0, -1e30)

    def columns(h):
        return pl.ds(pl.multiple_of(h * head, head), head)

    def grads(h, k_tile, v_tile, bias_tile, q_tile, g_tile, lse_tile, delta_tile):
        p = jnp.exp2(dot_nt(k_tile, q_tile) * (scale * LOG2E) + (bias_tile - lse_tile))
        ds = (p * (dot_nt(v_tile, g_tile) - delta_tile)).astype(jnp.bfloat16)
        return dot(ds, q_tile), dot(p.astype(jnp.bfloat16), g_tile), ds

    set_bias(0)
    k_t[...] = k_ref[...].astype(jnp.float32).T.astype(jnp.bfloat16)
    own_k[...] = jnp.zeros_like(own_k)
    own_v[...] = jnp.zeros_like(own_v)
    load_q.wait()
    load_g.wait()
    tile = LANES if rows % LANES == 0 else rows

    def own_head(h, carry):
        dq_t[columns(h), :] = jnp.zeros((head, rows), jnp.float32)
        for low in range(0, rows, tile):
            u = slice(low, low + tile)
            dk, dv, ds = grads(
                h,
                k_ref[u, :],
                v_ref[u, :],
                bias[u, low:],
                q[low:, columns(h)],
                g[low:, columns(h)],
                lse2[pl.ds(h, 1), :][:, low:],
                delta_ref[pl.ds(h, 1), :][:, low:],
            )
            own_k[u, :] += dk
            own_v[u, :] += dv
            dq_t[columns(h), low:] += dot(k_t[:, u], ds)
        return carry

    lax.fori_loop(0, heads, own_head, 0)

    def cross(d, carry):
        @pl.when(me >= d)
        def _():
            for copy in kv_copies(d):
                copy.wait_recv()
            set_bias(d)
            k_t[...] = kbuf[d - 1].astype(jnp.float32).T.astype(jnp.bfloat16)
            acc_k[...] = jnp.zeros_like(acc_k)
            acc_v[...] = jnp.zeros_like(acc_v)

            def one_head(h, inner):
                dk, dv, ds = grads(
                    h,
                    kbuf[d - 1],
                    vbuf[d - 1],
                    bias[...],
                    q[:, columns(h)],
                    g[:, columns(h)],
                    lse2[pl.ds(h, 1), :],
                    delta_ref[pl.ds(h, 1), :],
                )
                acc_k[...] += dk
                acc_v[...] += dv
                dq_t[columns(h), :] += dot(k_t[...], ds)
                return inner

            lax.fori_loop(0, heads, one_head, 0)
            out_k[d - 1] = (acc_k[...] * scale).astype(jnp.bfloat16)
            out_v[d - 1] = acc_v[...].astype(jnp.bfloat16)
            for copy in grad_copies(d):
                copy.start()

        return carry

    lax.fori_loop(1, REACH + 1, cross, 0)

    for h in range(heads):
        c = slice(h * head, (h + 1) * head)
        dq_ref[:, c] = (dq_t[c, :] * scale).T.astype(jnp.bfloat16)

    own_k[...] = own_k[...] * scale
    for d in range(1, REACH + 1):

        @pl.when(me + d < count)
        def _():
            for copy in grad_copies(d):
                copy.wait_recv()
            own_k[...] += in_k[d - 1].astype(jnp.float32)
            own_v[...] += in_v[d - 1].astype(jnp.float32)
            for copy in kv_copies(d):
                copy.wait_send()

        @pl.when(me >= d)
        def _():
            for copy in grad_copies(d):
                copy.wait_send()

    dk_ref[...] = own_k[...].astype(jnp.bfloat16)
    dv_ref[...] = own_v[...].astype(jnp.bfloat16)


def shards(count, per_seq, query_rows, key_rows, value_rows, out_grad, logsumexp, row_delta, doc_lengths):
    rows, head = key_rows.shape
    wide = query_rows.shape
    half, full = jnp.bfloat16, jnp.float32
    vmem = pl.BlockSpec(memory_space=pltpu.VMEM)
    hbm = pl.BlockSpec(memory_space=pl.ANY)
    return pl.pallas_call(
        functools.partial(kernel, count, per_seq),
        out_shape=(
            jax.ShapeDtypeStruct(wide, half),
            jax.ShapeDtypeStruct((rows, head), half),
            jax.ShapeDtypeStruct((rows, head), half),
        ),
        in_specs=[pl.BlockSpec(memory_space=pltpu.SMEM), hbm, hbm, vmem, vmem, vmem, vmem],
        out_specs=(vmem, vmem, vmem),
        scratch_shapes=[
            pltpu.VMEM(wide, half),
            pltpu.VMEM(wide, half),
            pltpu.VMEM((REACH, rows, head), half),
            pltpu.VMEM((REACH, rows, head), half),
            pltpu.VMEM((head, rows), half),
            pltpu.VMEM((rows, rows), full),
            pltpu.VMEM(logsumexp.shape, full),
            pltpu.VMEM((wide[1], rows), full),
            pltpu.VMEM((rows, head), full),
            pltpu.VMEM((rows, head), full),
            pltpu.VMEM((rows, head), full),
            pltpu.VMEM((rows, head), full),
            pltpu.VMEM((REACH, rows, head), half),
            pltpu.VMEM((REACH, rows, head), half),
            pltpu.VMEM((REACH, rows, head), half),
            pltpu.VMEM((REACH, rows, head), half),
            pltpu.SemaphoreType.DMA((2,)),
            pltpu.SemaphoreType.DMA((2, REACH)),
            pltpu.SemaphoreType.DMA((2, REACH)),
            pltpu.SemaphoreType.DMA((2, REACH)),
            pltpu.SemaphoreType.DMA((2, REACH)),
        ],
        compiler_params=pltpu.CompilerParams(collective_id=0, has_side_effects=True),
    )(doc_lengths, query_rows, out_grad, key_rows, value_rows, logsumexp, row_delta)


def solution(mesh):
    both = ("seq", "rep")
    count = mesh.shape["seq"] * mesh.shape["rep"]
    return jax.shard_map(
        functools.partial(shards, count, mesh.shape["rep"]),
        mesh=mesh,
        in_specs=(
            P(both, None),
            P(both, None),
            P(both, None),
            P(both, None),
            P(None, both),
            P(None, both),
            P(),
        ),
        out_specs=(P(both, None), P(both, None), P(both, None)),
        check_vma=False,
    )
```

```python
import functools
import math

import jax
import jax.numpy as jnp
from jax import lax
from jax.experimental import pallas as pl
from jax.experimental.pallas import tpu as pltpu
from jax.sharding import PartitionSpec as P

REACH = 4
LANES = 128
UNROLL = 2
LOG2E = math.log2(math.e)
MESH = pl.DeviceIdType.MESH


def dot(a, b):
    return jnp.dot(a, b, preferred_element_type=jnp.float32)


def dot_nt(a, b):
    return lax.dot_general(a, b, (((1,), (1,)), ((), ())), preferred_element_type=jnp.float32)


def kernel(
    count,
    per_seq,
    lens_ref,
    q_hbm,
    g_hbm,
    k_ref,
    v_ref,
    lse_ref,
    delta_ref,
    dq_ref,
    dk_ref,
    dv_ref,
    q,
    g,
    kbuf,
    vbuf,
    k_t,
    bias,
    lse2,
    dq_t,
    own_k,
    own_v,
    acc_k,
    acc_v,
    out_k,
    out_v,
    in_k,
    in_v,
    load_sem,
    kv_send,
    kv_recv,
    gr_send,
    gr_recv,
):
    rows, head = k_ref.shape
    heads = q_hbm.shape[1] // head
    pack = 2 if heads % 2 == 0 else 1
    scale = head**-0.5
    me = lax.axis_index("seq") * per_seq + lax.axis_index("rep")

    def device(index):
        return (lax.div(index, per_seq), lax.rem(index, per_seq))

    loads = [
        pltpu.make_async_copy(
            src.at[:, h * head : (h + 1) * head],
            dst.at[h * rows : (h + 1) * rows, :],
            load_sem.at[n, h],
        )
        for h in range(heads)
        for n, (src, dst) in enumerate(((q_hbm, q), (g_hbm, g)))
    ]
    for copy in loads:
        copy.start()

    barrier = pltpu.get_barrier_semaphore()
    for d in range(1, REACH + 1):

        @pl.when(me + d < count)
        def _():
            pl.semaphore_signal(barrier, inc=1, device_id=device(me + d), device_id_type=MESH)

        @pl.when(me >= d)
        def _():
            pl.semaphore_signal(barrier, inc=1, device_id=device(me - d), device_id_type=MESH)

    pl.semaphore_wait(barrier, jnp.minimum(me, REACH) + jnp.minimum(count - 1 - me, REACH))

    core = lax.rem(me, 2)
    partner = me + 1 - 2 * core

    def kv_copies(sources, d, target, order):
        return [
            pltpu.make_async_remote_copy(
                src_ref=src,
                dst_ref=dst.at[d - 1],
                send_sem=kv_send.at[n, order],
                recv_sem=kv_recv.at[n, d - 1],
                device_id=device(target),
                device_id_type=MESH,
            )
            for n, (src, dst) in enumerate(zip(sources, (kbuf, vbuf)))
        ]

    own = (k_ref, v_ref)
    routes = [
        (me + 2 < count, kv_copies(own, 2, me + 2, 0)),
        (me + 4 < count, kv_copies(own, 4, me + 4, 1)),
        (core == 0, kv_copies(own, 1, partner, 2)),
        ((core == 0) & (me >= 2), kv_copies((kbuf.at[1], vbuf.at[1]), 3, partner, 3)),
        ((core == 1) & (me >= 2), kv_copies((kbuf.at[1], vbuf.at[1]), 1, partner, 3)),
        ((core == 1) & (me >= 4), kv_copies((kbuf.at[3], vbuf.at[3]), 3, partner, 4)),
    ]

    def send(numbers):
        for number in numbers:

            @pl.when(routes[number][0])
            def _():
                for copy in routes[number][1]:
                    copy.start()

    def grad_copies(d):
        return [
            pltpu.make_async_remote_copy(
                src_ref=src.at[d - 1],
                dst_ref=dst.at[d - 1],
                send_sem=gr_send.at[n, d - 1],
                recv_sem=gr_recv.at[n, d - 1],
                device_id=device(me - d),
                device_id_type=MESH,
            )
            for n, (src, dst) in enumerate(((out_k, in_k), (out_v, in_v)))
        ]

    send((0, 1, 2))

    t_pos = me * rows + lax.broadcasted_iota(jnp.int32, (1, rows), 1)

    def next_doc(j, carry):
        end, start = carry
        end = end + lens_ref[j]
        return end, jnp.where(end <= t_pos, end, start)

    _, start = lax.fori_loop(
        0, lens_ref.shape[0], next_doc, (jnp.int32(0), jnp.zeros((1, rows), jnp.int32))
    )
    lse2[...] = lse_ref[...] * LOG2E

    def set_bias(d):
        u_pos = (me - d) * rows + lax.broadcasted_iota(jnp.int32, (rows, rows), 0)
        bias[...] = jnp.where((u_pos >= start) & (u_pos <= t_pos), 0.0, -1e30)

    def columns(h):
        return pl.ds(pl.multiple_of(h * head, head), head)

    def stacked(h):
        return pl.ds(pl.multiple_of(h * rows, rows), pack * rows)

    def head_rows(ref, h):
        return jnp.concatenate([ref[pl.ds(h + n, 1), :] for n in range(pack)], axis=1)

    def grads(k_tile, v_tile, bias_tile, q_tile, g_tile, lse_tile, delta_tile):
        p = jnp.exp2(dot_nt(k_tile, q_tile) * (scale * LOG2E) + (bias_tile - lse_tile))
        ds = (p * (dot_nt(v_tile, g_tile) - delta_tile)).astype(jnp.bfloat16)
        return dot(ds, q_tile), dot(p.astype(jnp.bfloat16), g_tile), ds

    set_bias(0)
    k_t[...] = k_ref[...].astype(jnp.float32).T.astype(jnp.bfloat16)
    own_k[...] = jnp.zeros_like(own_k)
    own_v[...] = jnp.zeros_like(own_v)
    for copy in loads:
        copy.wait()
    tile = LANES if rows % LANES == 0 else rows

    def own_head(h, carry):
        dq_t[columns(h), :] = jnp.zeros((head, rows), jnp.float32)
        for low in range(0, rows, tile):
            u = slice(low, low + tile)
            t = pl.ds(pl.multiple_of(h * rows + low, tile), rows - low)
            dk, dv, ds = grads(
                k_ref[u, :],
                v_ref[u, :],
                bias[u, low:],
                q[t, :],
                g[t, :],
                lse2[pl.ds(h, 1), :][:, low:],
                delta_ref[pl.ds(h, 1), :][:, low:],
            )
            own_k[u, :] += dk
            own_v[u, :] += dv
            dq_t[columns(h), low:] += dot(k_t[:, u], ds)
        return carry

    lax.fori_loop(0, heads, own_head, 0, unroll=2)

    def cross(step, carry):
        d = 2 * (step + 1) - lax.div(step, 2) * (4 * step - 5)

        @pl.when(me >= d)
        def _():
            for copy in kv_copies(own, d, partner, 0):
                copy.wait_recv()

            @pl.when(step == 0)
            def _():
                send((3, 4))

            @pl.when(step == 1)
            def _():
                send((5,))

            set_bias(d)
            k_t[...] = kbuf[d - 1].astype(jnp.float32).T.astype(jnp.bfloat16)
            acc_k[...] = jnp.zeros_like(acc_k)
            acc_v[...] = jnp.zeros_like(acc_v)

            def one_pack(n, inner):
                h = n * pack
                dk, dv, ds = grads(
                    kbuf[d - 1],
                    vbuf[d - 1],
                    jnp.concatenate([bias[...]] * pack, axis=1),
                    q[stacked(h), :],
                    g[stacked(h), :],
                    head_rows(lse2, h),
                    head_rows(delta_ref, h),
                )
                acc_k[...] += dk
                acc_v[...] += dv
                dq = dot(k_t[...], ds)
                for m in range(pack):
                    dq_t[columns(h + m), :] += dq[:, m * rows : (m + 1) * rows]
                return inner

            lax.fori_loop(0, heads // pack, one_pack, 0, unroll=UNROLL)
            out_k[d - 1] = (acc_k[...] * scale).astype(jnp.bfloat16)
            out_v[d - 1] = acc_v[...].astype(jnp.bfloat16)
            for copy in grad_copies(d):
                copy.start()

        return carry

    lax.fori_loop(0, REACH, cross, 0)

    for h in range(heads):
        c = slice(h * head, (h + 1) * head)
        dq_ref[:, c] = (dq_t[c, :] * scale).T.astype(jnp.bfloat16)

    own_k[...] = own_k[...] * scale
    for used, copies in routes:

        @pl.when(used)
        def _():
            for copy in copies:
                copy.wait_send()

    for d in (2, 4, 3, 1):

        @pl.when(me + d < count)
        def _():
            for copy in grad_copies(d):
                copy.wait_recv()
            own_k[...] += in_k[d - 1].astype(jnp.float32)
            own_v[...] += in_v[d - 1].astype(jnp.float32)
        @pl.when(me >= d)
        def _():
            for copy in grad_copies(d):
                copy.wait_send()

    dk_ref[...] = own_k[...].astype(jnp.bfloat16)
    dv_ref[...] = own_v[...].astype(jnp.bfloat16)


def shards(count, per_seq, query_rows, key_rows, value_rows, out_grad, logsumexp, row_delta, doc_lengths):
    rows, head = key_rows.shape
    wide = query_rows.shape
    heads = wide[1] // head
    half, full = jnp.bfloat16, jnp.float32
    vmem = pl.BlockSpec(memory_space=pltpu.VMEM)
    hbm = pl.BlockSpec(memory_space=pl.ANY)
    return pl.pallas_call(
        functools.partial(kernel, count, per_seq),
        out_shape=(
            jax.ShapeDtypeStruct(wide, half),
            jax.ShapeDtypeStruct((rows, head), half),
            jax.ShapeDtypeStruct((rows, head), half),
        ),
        in_specs=[pl.BlockSpec(memory_space=pltpu.SMEM), hbm, hbm, vmem, vmem, vmem, vmem],
        out_specs=(vmem, vmem, vmem),
        scratch_shapes=[
            pltpu.VMEM((heads * rows, head), half),
            pltpu.VMEM((heads * rows, head), half),
            pltpu.VMEM((REACH, rows, head), half),
            pltpu.VMEM((REACH, rows, head), half),
            pltpu.VMEM((head, rows), half),
            pltpu.VMEM((rows, rows), full),
            pltpu.VMEM(logsumexp.shape, full),
            pltpu.VMEM((wide[1], rows), full),
            pltpu.VMEM((rows, head), full),
            pltpu.VMEM((rows, head), full),
            pltpu.VMEM((rows, head), full),
            pltpu.VMEM((rows, head), full),
            pltpu.VMEM((REACH, rows, head), half),
            pltpu.VMEM((REACH, rows, head), half),
            pltpu.VMEM((REACH, rows, head), half),
            pltpu.VMEM((REACH, rows, head), half),
            pltpu.SemaphoreType.DMA((2, heads)),
            pltpu.SemaphoreType.DMA((2, 5)),
            pltpu.SemaphoreType.DMA((2, REACH)),
            pltpu.SemaphoreType.DMA((2, REACH)),
            pltpu.SemaphoreType.DMA((2, REACH)),
        ],
        compiler_params=pltpu.CompilerParams(collective_id=0, has_side_effects=True),
    )(doc_lengths, query_rows, out_grad, key_rows, value_rows, logsumexp, row_delta)


def solution(mesh):
    both = ("seq", "rep")
    count = mesh.shape["seq"] * mesh.shape["rep"]
    return jax.shard_map(
        functools.partial(shards, count, mesh.shape["rep"]),
        mesh=mesh,
        in_specs=(
            P(both, None),
            P(both, None),
            P(both, None),
            P(both, None),
            P(None, both),
            P(None, both),
            P(),
        ),
        out_specs=(P(both, None), P(both, None), P(both, None)),
        check_vma=False,
    )
```

```python
import functools
import math

import jax
import jax.numpy as jnp
from jax import lax
from jax.experimental import pallas as pl
from jax.experimental.pallas import tpu as pltpu
from jax.sharding import PartitionSpec as P

REACH = 4
LANES = 128
UNROLL = 4
LOG2E = math.log2(math.e)
MESH = pl.DeviceIdType.MESH


def dot(a, b):
    return jnp.dot(a, b, preferred_element_type=jnp.float32)


def dot_nt(a, b):
    return lax.dot_general(a, b, (((1,), (1,)), ((), ())), preferred_element_type=jnp.float32)


def kernel(
    count,
    per_seq,
    lens_ref,
    q_hbm,
    g_hbm,
    k_ref,
    v_ref,
    lse_ref,
    delta_ref,
    dq_ref,
    dk_ref,
    dv_ref,
    q,
    g,
    kbuf,
    vbuf,
    k_t,
    bias,
    lse2,
    dq_t,
    own_k,
    own_v,
    acc_k,
    acc_v,
    out_k,
    out_v,
    in_k,
    in_v,
    load_sem,
    kv_send,
    kv_recv,
    gr_send,
    gr_recv,
):
    rows, head = k_ref.shape
    heads = q_hbm.shape[1] // head
    pack = 2 if heads % 2 == 0 else 1
    scale = head**-0.5
    me = lax.axis_index("seq") * per_seq + lax.axis_index("rep")

    def device(index):
        return (lax.div(index, per_seq), lax.rem(index, per_seq))

    loads = [
        pltpu.make_async_copy(
            src.at[:, h * head : (h + 1) * head],
            dst.at[h * rows : (h + 1) * rows, :],
            load_sem.at[n, h],
        )
        for h in range(heads)
        for n, (src, dst) in enumerate(((q_hbm, q), (g_hbm, g)))
    ]
    for copy in loads:
        copy.start()

    barrier = pltpu.get_barrier_semaphore()
    for d in range(1, REACH + 1):

        @pl.when(me + d < count)
        def _():
            pl.semaphore_signal(barrier, inc=1, device_id=device(me + d), device_id_type=MESH)

        @pl.when(me >= d)
        def _():
            pl.semaphore_signal(barrier, inc=1, device_id=device(me - d), device_id_type=MESH)

    pl.semaphore_wait(barrier, jnp.minimum(me, REACH) + jnp.minimum(count - 1 - me, REACH))

    core = lax.rem(me, 2)
    partner = me + 1 - 2 * core

    def kv_copies(sources, d, target, order):
        return [
            pltpu.make_async_remote_copy(
                src_ref=src,
                dst_ref=dst.at[d - 1],
                send_sem=kv_send.at[n, order],
                recv_sem=kv_recv.at[n, d - 1],
                device_id=device(target),
                device_id_type=MESH,
            )
            for n, (src, dst) in enumerate(zip(sources, (kbuf, vbuf)))
        ]

    own = (k_ref, v_ref)
    routes = [
        (me + 2 < count, kv_copies(own, 2, me + 2, 0)),
        (me + 4 < count, kv_copies(own, 4, me + 4, 1)),
        (core == 0, kv_copies(own, 1, partner, 2)),
        ((core == 0) & (me >= 2), kv_copies((kbuf.at[1], vbuf.at[1]), 3, partner, 3)),
        ((core == 1) & (me >= 2), kv_copies((kbuf.at[1], vbuf.at[1]), 1, partner, 3)),
        ((core == 1) & (me >= 4), kv_copies((kbuf.at[3], vbuf.at[3]), 3, partner, 4)),
    ]

    def send(numbers):
        for number in numbers:

            @pl.when(routes[number][0])
            def _():
                for copy in routes[number][1]:
                    copy.start()

    def grad_copies(d):
        return [
            pltpu.make_async_remote_copy(
                src_ref=src.at[d - 1],
                dst_ref=dst.at[d - 1],
                send_sem=gr_send.at[n, d - 1],
                recv_sem=gr_recv.at[n, d - 1],
                device_id=device(me - d),
                device_id_type=MESH,
            )
            for n, (src, dst) in enumerate(((out_k, in_k), (out_v, in_v)))
        ]

    send((0, 1, 2))

    t_pos = me * rows + lax.broadcasted_iota(jnp.int32, (1, rows), 1)

    def next_doc(j, carry):
        end, start = carry
        end = end + lens_ref[j]
        return end, jnp.where(end <= t_pos, end, start)

    _, start = lax.fori_loop(
        0, lens_ref.shape[0], next_doc, (jnp.int32(0), jnp.zeros((1, rows), jnp.int32))
    )
    lse2[...] = lse_ref[...] * LOG2E

    def set_bias(d):
        u_pos = (me - d) * rows + lax.broadcasted_iota(jnp.int32, (rows, rows), 0)
        bias[...] = jnp.where((u_pos >= start) & (u_pos <= t_pos), 0.0, -1e30)

    def columns(h):
        return pl.ds(pl.multiple_of(h * head, head), head)

    def stacked(h):
        return pl.ds(pl.multiple_of(h * rows, rows), pack * rows)

    def head_rows(ref, h):
        return jnp.concatenate([ref[pl.ds(h + n, 1), :] for n in range(pack)], axis=1)

    def grads(k_tile, v_tile, bias_tile, q_tile, g_tile, lse_tile, delta_tile):
        p = jnp.exp2(dot_nt(k_tile, q_tile) * (scale * LOG2E) + (bias_tile - lse_tile))
        ds = (p * (dot_nt(v_tile, g_tile) - delta_tile)).astype(jnp.bfloat16)
        return dot(ds, q_tile), dot(p.astype(jnp.bfloat16), g_tile), ds

    set_bias(0)
    k_t[...] = k_ref[...].astype(jnp.float32).T.astype(jnp.bfloat16)
    own_k[...] = jnp.zeros_like(own_k)
    own_v[...] = jnp.zeros_like(own_v)
    for copy in loads:
        copy.wait()
    tile = LANES if rows % LANES == 0 else rows

    def own_head(h, carry):
        dq_t[columns(h), :] = jnp.zeros((head, rows), jnp.float32)
        for low in range(0, rows, tile):
            u = slice(low, low + tile)
            t = pl.ds(pl.multiple_of(h * rows + low, tile), rows - low)
            dk, dv, ds = grads(
                k_ref[u, :],
                v_ref[u, :],
                bias[u, low:],
                q[t, :],
                g[t, :],
                lse2[pl.ds(h, 1), :][:, low:],
                delta_ref[pl.ds(h, 1), :][:, low:],
            )
            own_k[u, :] += dk
            own_v[u, :] += dv
            dq_t[columns(h), low:] += dot(k_t[:, u], ds)
        return carry

    lax.fori_loop(0, heads, own_head, 0, unroll=2)

    def cross(step, carry):
        d = 2 * (step + 1) - lax.div(step, 2) * (4 * step - 5)

        @pl.when(me >= d)
        def _():
            for copy in kv_copies(own, d, partner, 0):
                copy.wait_recv()

            @pl.when(step == 0)
            def _():
                send((3, 4))

            @pl.when(step == 1)
            def _():
                send((5,))

            set_bias(d)
            k_t[...] = kbuf[d - 1].astype(jnp.float32).T.astype(jnp.bfloat16)
            acc_k[...] = jnp.zeros_like(acc_k)
            acc_v[...] = jnp.zeros_like(acc_v)

            def one_pack(n, inner):
                h = n * pack
                dk, dv, ds = grads(
                    kbuf[d - 1],
                    vbuf[d - 1],
                    jnp.concatenate([bias[...]] * pack, axis=1),
                    q[stacked(h), :],
                    g[stacked(h), :],
                    head_rows(lse2, h),
                    head_rows(delta_ref, h),
                )
                acc_k[...] += dk
                acc_v[...] += dv
                dq = dot(k_t[...], ds)
                for m in range(pack):
                    dq_t[columns(h + m), :] += dq[:, m * rows : (m + 1) * rows]
                return inner

            lax.fori_loop(0, heads // pack, one_pack, 0, unroll=UNROLL)
            out_k[d - 1] = (acc_k[...] * scale).astype(jnp.bfloat16)
            out_v[d - 1] = acc_v[...].astype(jnp.bfloat16)
            for copy in grad_copies(d):
                copy.start()

        return carry

    lax.fori_loop(0, REACH, cross, 0)

    for h in range(heads):
        c = slice(h * head, (h + 1) * head)
        dq_ref[:, c] = (dq_t[c, :] * scale).T.astype(jnp.bfloat16)

    own_k[...] = own_k[...] * scale
    for used, copies in routes:

        @pl.when(used)
        def _():
            for copy in copies:
                copy.wait_send()

    for d in (2, 4, 3, 1):

        @pl.when(me + d < count)
        def _():
            for copy in grad_copies(d):
                copy.wait_recv()
            own_k[...] += in_k[d - 1].astype(jnp.float32)
            own_v[...] += in_v[d - 1].astype(jnp.float32)
        @pl.when(me >= d)
        def _():
            for copy in grad_copies(d):
                copy.wait_send()

    dk_ref[...] = own_k[...].astype(jnp.bfloat16)
    dv_ref[...] = own_v[...].astype(jnp.bfloat16)


def pass_on(dq_ref, dk_ref, dv_ref, dq_out, dk_out, dv_out):
    dq_out[...] = dq_ref[...]
    dk_out[...] = dk_ref[...]
    dv_out[...] = dv_ref[...]


def shards(count, per_seq, query_rows, key_rows, value_rows, out_grad, logsumexp, row_delta, doc_lengths):
    rows, head = key_rows.shape
    wide = query_rows.shape
    heads = wide[1] // head
    half, full = jnp.bfloat16, jnp.float32
    vmem = pl.BlockSpec(memory_space=pltpu.VMEM)
    hbm = pl.BlockSpec(memory_space=pl.ANY)
    grads = pl.pallas_call(
        functools.partial(kernel, count, per_seq),
        out_shape=(
            jax.ShapeDtypeStruct(wide, half),
            jax.ShapeDtypeStruct((rows, head), half),
            jax.ShapeDtypeStruct((rows, head), half),
        ),
        in_specs=[pl.BlockSpec(memory_space=pltpu.SMEM), hbm, hbm, vmem, vmem, vmem, vmem],
        out_specs=(vmem, vmem, vmem),
        scratch_shapes=[
            pltpu.VMEM((heads * rows, head), half),
            pltpu.VMEM((heads * rows, head), half),
            pltpu.VMEM((REACH, rows, head), half),
            pltpu.VMEM((REACH, rows, head), half),
            pltpu.VMEM((head, rows), half),
            pltpu.VMEM((rows, rows), full),
            pltpu.VMEM(logsumexp.shape, full),
            pltpu.VMEM((wide[1], rows), full),
            pltpu.VMEM((rows, head), full),
            pltpu.VMEM((rows, head), full),
            pltpu.VMEM((rows, head), full),
            pltpu.VMEM((rows, head), full),
            pltpu.VMEM((REACH, rows, head), half),
            pltpu.VMEM((REACH, rows, head), half),
            pltpu.VMEM((REACH, rows, head), half),
            pltpu.VMEM((REACH, rows, head), half),
            pltpu.SemaphoreType.DMA((2, heads)),
            pltpu.SemaphoreType.DMA((2, 5)),
            pltpu.SemaphoreType.DMA((2, REACH)),
            pltpu.SemaphoreType.DMA((2, REACH)),
            pltpu.SemaphoreType.DMA((2, REACH)),
        ],
        compiler_params=pltpu.CompilerParams(collective_id=0, has_side_effects=True),
    )(doc_lengths, query_rows, out_grad, key_rows, value_rows, logsumexp, row_delta)
    return pl.pallas_call(
        pass_on,
        out_shape=tuple(jax.ShapeDtypeStruct(part.shape, part.dtype) for part in grads),
        in_specs=[vmem] * 3,
        out_specs=(vmem,) * 3,
    )(*grads)


def solution(mesh):
    both = ("seq", "rep")
    count = mesh.shape["seq"] * mesh.shape["rep"]
    return jax.shard_map(
        functools.partial(shards, count, mesh.shape["rep"]),
        mesh=mesh,
        in_specs=(
            P(both, None),
            P(both, None),
            P(both, None),
            P(both, None),
            P(None, both),
            P(None, both),
            P(),
        ),
        out_specs=(P(both, None), P(both, None), P(both, None)),
        check_vma=False,
    )
```
